32 devices in a mesh: data: 1 (over z), inner: 4 (over y), stage: 8 (over x, core).
Axes of the slice: x: 4, y: 4, z: 1, core: 2. Of those that a mesh axis runs over, the one named last changes fastest.
The devices are a block of a 4x4x8 slice.
Arguments:
- x: bfloat16 [64, 128, 768], P(('data', 'stage', 'inner'))
- g: bfloat16 [64, 128, 768], P(('data', 'stage', 'inner'))
- w1: bfloat16 [1, 8, 1, 768, 3072], P(None, 'stage', None, None, 'inner')
- w2: bfloat16 [1, 8, 1, 3072, 768], P(None, 'stage', None, 'inner')
Outputs:
- output 1: bfloat16 [64, 128, 768], P(('data', 'stage', 'inner'))
- output 2: bfloat16 [64, 128, 768], P(('data', 'stage', 'inner'))
- output 3: float32 [1, 8, 1, 768, 3072], P('data', 'stage', None, None, 'inner')
- output 4: float32 [1, 8, 1, 3072, 768], P('data', 'stage', None, 'inner')
All inputs are finite; a program needn't handle non-finite values.
Results may differ from the reference program's by a relative error of at most 0.0156898.
Values are sent between devices in bfloat16 or wider.
A program may use at most 768 MiB of HBM per device.

```python
import jax
import jax.numpy as jnp
from jax import lax

D = 768
FF = 3072
V = 1
STAGE = 8
INNER = 4
K = 1
MD = 2
B = 128

M = STAGE * INNER * MD
L = V * STAGE * K


def setup_inputs(seed: int = 0, part: int = 0) -> dict:
    key = jax.random.PRNGKey(seed)
    kw1, kw2, kd = jax.random.split(key, 3)
    kx, kg = jax.random.split(jax.random.fold_in(kd, part), 2)
    w1 = jax.random.normal(kw1, (V, STAGE, K, D, FF), jnp.float32) * D ** -0.5
    w2 = jax.random.normal(kw2, (V, STAGE, K, FF, D), jnp.float32) * (2.0 / (FF * L)) ** 0.5
    x = jax.random.normal(kx, (M, B, D), jnp.float32)
    g = jax.random.normal(kg, (M, B, D), jnp.float32)
    return {'x': x.astype(jnp.bfloat16), 'g': g.astype(jnp.bfloat16), 'w1': w1.astype(jnp.bfloat16), 'w2': w2.astype(jnp.bfloat16)}


def _gelu(u):
    return jax.nn.gelu(u, approximate=True)


def reference(x, g, w1, w2):
    w1s = w1.reshape(L, D, FF)
    w2s = w2.reshape(L, FF, D)

    def fwd(h, w):
        a1, a2 = w
        u = jnp.dot(h, a1, preferred_element_type=jnp.float32)
        a = _gelu(u).astype(jnp.bfloat16)
        hn = (h.astype(jnp.float32) + jnp.dot(a, a2, preferred_element_type=jnp.float32)).astype(jnp.bfloat16)
        return hn, h

    y, hs = lax.scan(fwd, x.reshape(M * B, D), (w1s, w2s))

    def bwd(dh, inp):
        h, a1, a2 = inp
        u = jnp.dot(h, a1, preferred_element_type=jnp.float32)
        gv, gvjp = jax.vjp(_gelu, u)
        a = gv.astype(jnp.bfloat16)
        e = jnp.dot(dh, a2.T, preferred_element_type=jnp.float32)
        du = gvjp(e)[0].astype(jnp.bfloat16)
        dw2 = jnp.dot(a.T, dh, preferred_element_type=jnp.float32)
        dw1 = jnp.dot(h.T, du, preferred_element_type=jnp.float32)
        dhn = (dh.astype(jnp.float32) + jnp.dot(du, a1.T, preferred_element_type=jnp.float32)).astype(jnp.bfloat16)
        return dhn, (dw1, dw2)

    dx, (dw1, dw2) = lax.scan(bwd, g.reshape(M * B, D), (hs, w1s, w2s), reverse=True)
    return (y.reshape(M, B, D), dx.reshape(M, B, D), dw1.reshape(V, STAGE, K, D, FF), dw2.reshape(V, STAGE, K, FF, D))
```

```python
import functools

import jax
import jax.numpy as jnp
from jax import lax
from jax.experimental import pallas as pl
from jax.experimental.pallas import tpu as pltpu
from jax.sharding import PartitionSpec as P

MESH = pl.DeviceIdType.MESH
F32 = jnp.float32
BF16 = jnp.bfloat16
C0 = 0.7978845608
C1 = 0.044715


def _dot(a, b):
    return jnp.dot(a, b, preferred_element_type=F32)


def _dot_t(a, b):
    return lax.dot_general(a, b, (((1,), (1,)), ((), ())), preferred_element_type=F32)


def _remote(src, dst, ssem, rsem, dev):
    return pltpu.make_async_remote_copy(src_ref=src, dst_ref=dst, send_sem=ssem, recv_sem=rsem, device_id=dev, device_id_type=MESH)


def _pipe_kernel(ns, ni, md, x_ref, g_ref, w1_ref, w2_ref,
                 y_ref, dx_ref, ht_ref, gt_ref, a_ref, du_ref, gp_ref,
                 w1f, w2f, hbuf, gbuf, hout, gout, htv, gtv, abuf, dubuf, gpbuf,
                 wsend, wrecv, wloc, xsend, hrecv, grecv, hsend, gsend, yrecv, dxrecv,
                 htsem, gtsem, asem, dusem, gpsem):
    s = lax.axis_index('stage')
    i = lax.axis_index('inner')
    n = ns * md
    b = x_ref.shape[1]
    right = lax.rem(i + 1, ni)
    left = lax.rem(i + ni - 1, ni)
    opp = lax.rem(i + 2, ni)

    barrier = pltpu.get_barrier_semaphore()
    for k in range(1, ns):
        pl.semaphore_signal(barrier, inc=1, device_id={'stage': lax.rem(s + k, ns)}, device_id_type=MESH)
    for nb in (left, right):
        pl.semaphore_signal(barrier, inc=1, device_id={'inner': nb}, device_id_type=MESH)

    own1 = pltpu.make_async_copy(w1_ref, w1f.at[i], wloc.at[0])
    own2 = pltpu.make_async_copy(w2_ref, w2f.at[i], wloc.at[1])
    own1.start()
    own2.start()
    pl.semaphore_wait(barrier, ns + 1)

    rs = [_remote(w1_ref, w1f.at[i], wsend.at[0], wrecv.at[0], {'inner': right}),
          _remote(w2_ref, w2f.at[i], wsend.at[1], wrecv.at[1], {'inner': right})]
    ls = [_remote(w2_ref, w2f.at[i], wsend.at[3], wrecv.at[3], {'inner': left}),
          _remote(w1_ref, w1f.at[i], wsend.at[4], wrecv.at[4], {'inner': left})]
    rs[0].start()
    ls[0].start()
    rs[1].start()
    ls[1].start()

    for k in range(md):
        m = s * md + k

        @pl.when(s == 0)
        def _():
            pltpu.make_async_copy(x_ref.at[k], hbuf.at[m], hrecv.at[m]).start()

        @pl.when(s != 0)
        def _():
            _remote(x_ref.at[k], hbuf.at[m], xsend.at[k], hrecv.at[m], {'stage': 0}).start()

    for k in range(md):
        m = s * md + k

        @pl.when(s == ns - 1)
        def _():
            pltpu.make_async_copy(g_ref.at[k], gbuf.at[m], grecv.at[m]).start()

        @pl.when(s != ns - 1)
        def _():
            _remote(g_ref.at[k], gbuf.at[m], xsend.at[md + k], grecv.at[m], {'stage': ns - 1}).start()

    pltpu.make_async_copy(w1f.at[left], w1f.at[left], wrecv.at[0]).wait()
    fr = _remote(w1f.at[left], w1f.at[left], wsend.at[2], wrecv.at[2], {'inner': right})
    fr.start()
    pltpu.make_async_copy(w2f.at[right], w2f.at[right], wrecv.at[3]).wait()
    fl = _remote(w2f.at[right], w2f.at[right], wsend.at[5], wrecv.at[5], {'inner': left})
    fl.start()
    own1.wait()
    own2.wait()
    pltpu.make_async_copy(w2f.at[left], w2f.at[left], wrecv.at[1]).wait()
    pltpu.make_async_copy(w1f.at[right], w1f.at[right], wrecv.at[4]).wait()
    pltpu.make_async_copy(w1f.at[opp], w1f.at[opp], wrecv.at[2]).wait()
    pltpu.make_async_copy(w2f.at[opp], w2f.at[opp], wrecv.at[5]).wait()

    def fwd(m, c):
        slot = lax.rem(m, 2)
        col = pl.ds(pl.multiple_of(m * b, b), b)
        pltpu.make_async_copy(hbuf.at[m], hbuf.at[m], hrecv.at[m]).wait()

        @pl.when(m >= 2)
        def _():
            pltpu.make_async_copy(abuf.at[slot], a_ref.at[:, m - 2], asem.at[slot]).wait()
            pltpu.make_async_copy(gpbuf.at[slot], gp_ref.at[:, m - 2], gpsem.at[slot]).wait()

        h = hbuf[m]
        for q in range(ni):
            u = _dot(h, w1f[q])
            u2 = u * u
            t = jnp.tanh(u * (C0 + (C0 * C1) * u2))
            p = 0.5 + 0.5 * t
            hu = 0.5 * u
            abuf[slot, q] = (u * p).astype(BF16)
            gpbuf[slot, q] = p + hu * (1.0 - t * t) * (C0 + (3.0 * C0 * C1) * u2)
        acc = _dot(abuf[slot, 0], w2f[0])
        for q in range(1, ni):
            acc = acc + _dot(abuf[slot, q], w2f[q])
        hout[m] = (h.astype(F32) + acc).astype(BF16)
        home = m // md
        kk = lax.rem(m, md)

        @pl.when(s < ns - 1)
        def _():
            _remote(hout.at[m], hbuf.at[m], hsend, hrecv.at[m], {'stage': lax.rem(s + 1, ns)}).start()

        @pl.when((s == ns - 1) & (home != ns - 1))
        def _():
            _remote(hout.at[m], y_ref.at[kk], hsend, yrecv.at[kk], {'stage': home}).start()

        @pl.when((s == ns - 1) & (home == ns - 1))
        def _():
            pltpu.make_async_copy(hout.at[m], y_ref.at[kk], hsend).start()

        pltpu.make_async_copy(abuf.at[slot], a_ref.at[:, m], asem.at[slot]).start()
        pltpu.make_async_copy(gpbuf.at[slot], gp_ref.at[:, m], gpsem.at[slot]).start()
        htv[:, col] = h.T
        pltpu.make_async_copy(htv.at[:, col], ht_ref.at[:, col], htsem).start()
        return c

    lax.fori_loop(0, n, fwd, 0)
    for k in range(2):
        pltpu.make_async_copy(abuf.at[k], a_ref.at[:, n - 2 + k], asem.at[k]).wait()
        pltpu.make_async_copy(gpbuf.at[k], gp_ref.at[:, n - 2 + k], gpsem.at[k]).wait()
    for k in range(2):
        pltpu.make_async_copy(gp_ref.at[:, k], gpbuf.at[k], gpsem.at[k]).start()

    def bwd(m, c):
        slot = lax.rem(m, 2)
        col = pl.ds(pl.multiple_of(m * b, b), b)
        pltpu.make_async_copy(gp_ref.at[:, m], gpbuf.at[slot], gpsem.at[slot]).wait()
        pltpu.make_async_copy(gbuf.at[m], gbuf.at[m], grecv.at[m]).wait()

        @pl.when(m >= 2)
        def _():
            pltpu.make_async_copy(dubuf.at[slot], du_ref.at[:, m - 2], dusem.at[slot]).wait()

        g = gbuf[m]
        for q in range(ni):
            e = _dot_t(g, w2f[q])
            dubuf[slot, q] = (e * gpbuf[slot, q]).astype(BF16)
        acc = _dot_t(dubuf[slot, 0], w1f[0])
        for q in range(1, ni):
            acc = acc + _dot_t(dubuf[slot, q], w1f[q])
        gout[m] = (g.astype(F32) + acc).astype(BF16)
        home = m // md
        kk = lax.rem(m, md)

        @pl.when(s > 0)
        def _():
            _remote(gout.at[m], gbuf.at[m], gsend, grecv.at[m], {'stage': lax.rem(s + ns - 1, ns)}).start()

        @pl.when((s == 0) & (home != 0))
        def _():
            _remote(gout.at[m], dx_ref.at[kk], gsend, dxrecv.at[kk], {'stage': home}).start()

        @pl.when((s == 0) & (home == 0))
        def _():
            pltpu.make_async_copy(gout.at[m], dx_ref.at[kk], gsend).start()

        pltpu.make_async_copy(dubuf.at[slot], du_ref.at[:, m], dusem.at[slot]).start()

        @pl.when(m < n - 2)
        def _():
            pltpu.make_async_copy(gp_ref.at[:, m + 2], gpbuf.at[slot], gpsem.at[slot]).start()

        gtv[:, col] = g.T
        pltpu.make_async_copy(gtv.at[:, col], gt_ref.at[:, col], gtsem).start()
        return c

    lax.fori_loop(0, n, bwd, 0)

    for k in range(2):
        pltpu.make_async_copy(dubuf.at[k], du_ref.at[:, n - 2 + k], dusem.at[k]).wait()
    pltpu.make_async_copy(htv, ht_ref, htsem).wait()
    pltpu.make_async_copy(gtv, gt_ref, gtsem).wait()
    pltpu.make_async_copy(hout, hout, hsend).wait()
    pltpu.make_async_copy(gout, gout, gsend).wait()
    for r in rs + ls + [fr, fl]:
        r.wait_send()
    for k in range(md):
        @pl.when(s != 0)
        def _():
            pltpu.make_async_copy(x_ref.at[k], x_ref.at[k], xsend.at[k]).wait()
            pltpu.make_async_copy(dx_ref.at[k], dx_ref.at[k], dxrecv.at[k]).wait()

        @pl.when(s != ns - 1)
        def _():
            pltpu.make_async_copy(g_ref.at[k], g_ref.at[k], xsend.at[md + k]).wait()
            pltpu.make_async_copy(y_ref.at[k], y_ref.at[k], yrecv.at[k]).wait()


def _wgrad_kernel(ni, nr, ht_ref, gt_ref, a_ref, du_ref, o1_ref, o2_ref,
                  hv, gv, dv, av, s1, s2, r1, r2,
                  lsem, dsem, snd1, snd2, rcv1, rcv2):
    i = lax.axis_index('inner')
    right = lax.rem(i + 1, ni)
    left = lax.rem(i + ni - 1, ni)
    barrier = pltpu.get_barrier_semaphore()
    for nb in (left, right):
        pl.semaphore_signal(barrier, inc=1, device_id={'inner': nb}, device_id_type=MESH)
    ch = pltpu.make_async_copy(ht_ref, hv, lsem.at[0])
    cg = pltpu.make_async_copy(gt_ref, gv, lsem.at[1])

    def loads(t):
        c1 = lax.rem(i + 2 * ni - 1 - t, ni)
        c2 = lax.rem(i + 1 + t, ni)
        return (pltpu.make_async_copy(du_ref.at[c1], dv.at[t % 2], dsem.at[0, t % 2]),
                pltpu.make_async_copy(a_ref.at[c2], av.at[t % 2], dsem.at[1, t % 2]))

    cps = loads(0)
    ch.start()
    cps[0].start()
    cg.start()
    cps[1].start()
    pl.semaphore_wait(barrier, 2)
    rows = s1.shape[1]
    k = dv.shape[1] * dv.shape[2]
    d = dv.shape[3]
    for t in range(ni):
        nxt = loads(t + 1) if t + 1 < ni else None
        if nxt is not None:
            nxt[0].start()
            nxt[1].start()
        if t == 0:
            ch.wait()
        cps[0].wait()
        if t == 0:
            cg.wait()
        cps[1].wait()
        slot = t % 2

        def block(r, c):
            row = pl.ds(pl.multiple_of(r * rows, rows), rows)
            p1 = _dot(hv[row, :], dv[slot].reshape(k, d))
            if t == 0:
                src1 = s1.at[r]
                s1[r] = p1
            else:
                src1 = r1.at[t - 1, r]
                pltpu.make_async_copy(src1, src1, rcv1.at[t - 1, r]).wait()
                if t < ni - 1:
                    r1[t - 1, r] = r1[t - 1, r] + p1
                else:
                    o1_ref[row, :] = r1[t - 1, r] + p1
            if t < ni - 1:
                _remote(src1, r1.at[t, r], snd1, rcv1.at[t, r], {'inner': right}).start()
            p2 = _dot(gv[row, :], av[slot].reshape(k, d))
            if t == 0:
                src2 = s2.at[r]
                s2[r] = p2
            else:
                src2 = r2.at[t - 1, r]
                pltpu.make_async_copy(src2, src2, rcv2.at[t - 1, r]).wait()
                if t < ni - 1:
                    r2[t - 1, r] = r2[t - 1, r] + p2
                else:
                    o2_ref[:, row] = (r2[t - 1, r] + p2).T
            if t < ni - 1:
                _remote(src2, r2.at[t, r], snd2, rcv2.at[t, r], {'inner': left}).start()
            return c

        lax.fori_loop(0, nr, block, 0)
        cps = nxt
    for sem in (snd1, snd2):
        pltpu.make_async_copy(r1, r1, sem).wait()


def solution(mesh):
    ns = mesh.shape['stage']
    ni = mesh.shape['inner']
    act = P(('data', 'stage', 'inner'), None, None)
    s1 = P(None, 'stage', None, None, 'inner')
    s2 = P(None, 'stage', None, 'inner', None)
    o1 = P('data', 'stage', None, None, 'inner')
    o2 = P('data', 'stage', None, 'inner', None)
    any_ = pl.BlockSpec(memory_space=pl.ANY)
    vmem = pl.BlockSpec(memory_space=pltpu.VMEM)
    dma = pltpu.SemaphoreType.DMA

    def body(x, g, w1, w2):
        md, b, d = x.shape
        f = w1.shape[-1]
        n = ns * md
        sds = jax.ShapeDtypeStruct
        y, dx, ht, gt, a, du, _ = pl.pallas_call(
            functools.partial(_pipe_kernel, ns, ni, md),
            out_shape=(sds((md, b, d), BF16), sds((md, b, d), BF16), sds((d, n * b), BF16), sds((d, n * b), BF16),
                       sds((ni, n, b, f), BF16), sds((ni, n, b, f), BF16), sds((ni, n, b, f), F32)),
            in_specs=[any_] * 4,
            out_specs=(any_,) * 7,
            scratch_shapes=[
                pltpu.VMEM((ni, d, f), BF16), pltpu.VMEM((ni, f, d), BF16),
                pltpu.VMEM((n, b, d), BF16), pltpu.VMEM((n, b, d), BF16),
                pltpu.VMEM((n, b, d), BF16), pltpu.VMEM((n, b, d), BF16),
                pltpu.VMEM((d, n * b), BF16), pltpu.VMEM((d, n * b), BF16),
                pltpu.VMEM((2, ni, b, f), BF16), pltpu.VMEM((2, ni, b, f), BF16),
                pltpu.VMEM((2, ni, b, f), F32),
                dma((6,)), dma((6,)), dma((2,)), dma((2 * md,)), dma((n,)), dma((n,)),
                dma(()), dma(()), dma((md,)), dma((md,)),
                dma(()), dma(()), dma((2,)), dma((2,)), dma((2,)),
            ],
            compiler_params=pltpu.CompilerParams(collective_id=0, has_side_effects=True, vmem_limit_bytes=60 * 2**20),
            name='pipe',
        )(x, g, w1[0, 0, 0], w2[0, 0, 0])
        nr = d // b
        dw1, dw2 = pl.pallas_call(
            functools.partial(_wgrad_kernel, ni, nr),
            out_shape=(sds((d, f), F32), sds((f, d), F32)),
            in_specs=[any_] * 4,
            out_specs=(vmem, vmem),
            scratch_shapes=[
                pltpu.VMEM((d, n * b), BF16), pltpu.VMEM((d, n * b), BF16),
                pltpu.VMEM((2, n, b, f), BF16), pltpu.VMEM((2, n, b, f), BF16),
                pltpu.VMEM((nr, b, f), F32), pltpu.VMEM((nr, b, f), F32),
                pltpu.VMEM((ni - 1, nr, b, f), F32), pltpu.VMEM((ni - 1, nr, b, f), F32),
                dma((2,)), dma((2, 2)), dma(()), dma(()),
                dma((ni - 1, nr)), dma((ni - 1, nr)),
            ],
            compiler_params=pltpu.CompilerParams(collective_id=1, has_side_effects=True, vmem_limit_bytes=60 * 2**20),
            name='wgrad',
        )(ht, gt, a, du)
        return y, dx, dw1[None, None, None], dw2[None, None, None]

    return jax.shard_map(body, mesh=mesh, in_specs=(act, act, s1, s2), out_specs=(act, act, o1, o2), check_vma=False)
```

```python
import functools

import jax
import jax.numpy as jnp
from jax import lax
from jax.experimental import pallas as pl
from jax.experimental.pallas import tpu as pltpu
from jax.sharding import PartitionSpec as P

MESH = pl.DeviceIdType.MESH
F32 = jnp.float32
BF16 = jnp.bfloat16
C0 = 0.7978845608
C1 = 0.044715


def _dot(a, b):
    return jnp.dot(a, b, preferred_element_type=F32)


def _dot_t(a, b):
    return lax.dot_general(a, b, (((1,), (1,)), ((), ())), preferred_element_type=F32)


def _gate(u):
    return 0.5 + 0.5 * jnp.tanh(u * (C0 + (C0 * C1) * (u * u)))


def _slope(u, p):
    return p * (1.0 + ((1.0 - p) * u) * (2.0 * C0 + (6.0 * C0 * C1) * (u * u)))


def _remote(src, dst, ssem, rsem, dev):
    return pltpu.make_async_remote_copy(src_ref=src, dst_ref=dst, send_sem=ssem, recv_sem=rsem, device_id=dev, device_id_type=MESH)


def _pipe_kernel(ns, ni, md, x_ref, g_ref, w1_ref, w2_ref,
                 y_ref, dx_ref, hg_ref, a_ref, du_ref,
                 w1f, w2f, w1t, w2t, hbuf, gbuf, gp, htb, gtb, abuf, dubuf,
                 wsend, wrecv, wloc, xsend, hrecv, grecv, hsend, gsend, yrecv, dxrecv,
                 htsem, gtsem, asem, dusem, ygo):
    s = lax.axis_index('stage')
    i = lax.axis_index('inner')
    n = ns * md
    b, d = x_ref.shape[1:]
    f = w1_ref.shape[1]
    right = lax.rem(i + 1, ni)
    left = lax.rem(i + ni - 1, ni)
    opp = lax.rem(i + 2, ni)

    barrier = pltpu.get_barrier_semaphore()
    for k in range(1, ns):
        pl.semaphore_signal(barrier, inc=1, device_id={'stage': lax.rem(s + k, ns)}, device_id_type=MESH)
    for nb in (left, right):
        pl.semaphore_signal(barrier, inc=1, device_id={'inner': nb}, device_id_type=MESH)

    own1 = pltpu.make_async_copy(w1_ref, w1f.at[i], wloc.at[0])
    own2 = pltpu.make_async_copy(w2_ref, w2f.at[i], wloc.at[1])
    own1.start()
    own2.start()
    pl.semaphore_wait(barrier, ns + 1)

    rs = [_remote(w1_ref, w1f.at[i], wsend.at[0], wrecv.at[0], {'inner': right}),
          _remote(w2_ref, w2f.at[i], wsend.at[1], wrecv.at[1], {'inner': right})]
    ls = [_remote(w2_ref, w2f.at[i], wsend.at[3], wrecv.at[3], {'inner': left}),
          _remote(w1_ref, w1f.at[i], wsend.at[4], wrecv.at[4], {'inner': left})]
    rs[0].start()
    ls[0].start()
    rs[1].start()
    ls[1].start()

    for k in range(md):
        m = s * md + k

        @pl.when(s == 0)
        def _():
            pltpu.make_async_copy(x_ref.at[k], hbuf.at[m], hrecv.at[m]).start()

        @pl.when(s != 0)
        def _():
            _remote(x_ref.at[k], hbuf.at[m], xsend.at[k], hrecv.at[m], {'stage': 0}).start()

    for k in range(md):
        m = s * md + k

        @pl.when(s == ns - 1)
        def _():
            pltpu.make_async_copy(g_ref.at[k], gbuf.at[m], grecv.at[m]).start()

        @pl.when(s != ns - 1)
        def _():
            _remote(g_ref.at[k], gbuf.at[m], xsend.at[md + k], grecv.at[m], {'stage': ns - 1}).start()

    def turn(k):
        w1t[k] = w1f[k].T
        w2t[k] = w2f[k].T

    own1.wait()
    own2.wait()
    turn(i)
    pltpu.make_async_copy(w1f.at[left], w1f.at[left], wrecv.at[0]).wait()
    fr = _remote(w1f.at[left], w1f.at[left], wsend.at[2], wrecv.at[2], {'inner': right})
    fr.start()
    pltpu.make_async_copy(w2f.at[right], w2f.at[right], wrecv.at[3]).wait()
    fl = _remote(w2f.at[right], w2f.at[right], wsend.at[5], wrecv.at[5], {'inner': left})
    fl.start()
    pltpu.make_async_copy(w2f.at[left], w2f.at[left], wrecv.at[1]).wait()
    turn(left)
    pltpu.make_async_copy(w1f.at[right], w1f.at[right], wrecv.at[4]).wait()
    turn(right)
    pltpu.make_async_copy(w1f.at[opp], w1f.at[opp], wrecv.at[2]).wait()
    pltpu.make_async_copy(w2f.at[opp], w2f.at[opp], wrecv.at[5]).wait()

    @pl.when(s >= 2)
    def _():
        turn(opp)

    nc = 256

    def fwd_in(m):
        slot = lax.rem(m, 2)
        pltpu.make_async_copy(hbuf.at[m], hbuf.at[m], hrecv.at[m]).wait()

        @pl.when(m >= 2)
        def _():
            pltpu.make_async_copy(abuf.at[slot], a_ref.at[:, m - 2], asem.at[slot]).wait()
            pltpu.make_async_copy(htb.at[slot], htb.at[slot], htsem.at[slot]).wait()

    def fwd_math(m):
        slot = lax.rem(m, 2)
        h = hbuf[m]
        htb[slot] = h.T
        accs = [None] * (d // nc)

        def down(q):
            for c in range(d // nc):
                r = _dot(abuf[slot, q], w2f[q, :, c * nc:(c + 1) * nc])
                accs[c] = r if q == 0 else accs[c] + r

        for q in range(ni):
            for c in range(f // nc):
                cs = slice(c * nc, (c + 1) * nc)
                u = _dot(h, w1f[q, :, cs])
                p = _gate(u)
                abuf[slot, q, :, cs] = (u * p).astype(BF16)
                gp[m, q, :, cs] = _slope(u, p) if q < ni // 2 else u
            if q > 0:
                down(q - 1)
            yield
        down(ni - 1)
        for c in range(d // nc):
            cs = slice(c * nc, (c + 1) * nc)
            hbuf[m, :, cs] = (h[:, cs].astype(F32) + accs[c]).astype(BF16)

    def fwd_out(m):
        slot = lax.rem(m, 2)
        col = pl.ds(pl.multiple_of(m * b, b), b)
        home = m // md
        kk = lax.rem(m, md)

        @pl.when(s < ns - 1)
        def _():
            _remote(hbuf.at[m], hbuf.at[m], hsend, hrecv.at[m], {'stage': lax.rem(s + 1, ns)}).start()

        @pl.when((s == ns - 1) & ((home == ns - 2) | (home < 2)))
        def _():
            _remote(hbuf.at[m], y_ref.at[kk], hsend, yrecv.at[kk], {'stage': home}).start()

        @pl.when((s == ns - 1) & (home == ns - 1))
        def _():
            pltpu.make_async_copy(hbuf.at[m], y_ref.at[kk], hsend).start()

        pltpu.make_async_copy(abuf.at[slot], a_ref.at[:, m], asem.at[slot]).start()
        pltpu.make_async_copy(htb.at[slot], hg_ref.at[0, :, col], htsem.at[slot]).start()

    def bwd_in(m):
        slot = lax.rem(m, 2)
        pltpu.make_async_copy(gbuf.at[m], gbuf.at[m], grecv.at[m]).wait()

        @pl.when((s == ns - 3) & (m == n - 1))
        def _():
            pl.semaphore_signal(ygo, inc=1, device_id={'stage': ns - 1}, device_id_type=MESH)

        @pl.when(m >= 2)
        def _():
            pltpu.make_async_copy(dubuf.at[slot], du_ref.at[:, m - 2], dusem.at[slot]).wait()
            pltpu.make_async_copy(gtb.at[slot], gtb.at[slot], gtsem.at[slot]).wait()

    def bwd_math(m):
        slot = lax.rem(m, 2)
        g = gbuf[m]
        gtb[slot] = g.T
        accs = [None] * (d // nc)

        def down(q):
            for c in range(d // nc):
                r = _dot(dubuf[slot, q], w1t[q, :, c * nc:(c + 1) * nc])
                accs[c] = r if q == 0 else accs[c] + r

        for q in range(ni):
            for c in range(f // nc):
                cs = slice(c * nc, (c + 1) * nc)
                e = _dot(g, w2t[q, :, cs])
                v = gp[m, q, :, cs]
                if q >= ni // 2:
                    v = _slope(v, _gate(v))
                dubuf[slot, q, :, cs] = (e * v).astype(BF16)
            if q > 0:
                down(q - 1)
            yield
        down(ni - 1)
        for c in range(d // nc):
            cs = slice(c * nc, (c + 1) * nc)
            gbuf[m, :, cs] = (g[:, cs].astype(F32) + accs[c]).astype(BF16)

    def bwd_out(m):
        slot = lax.rem(m, 2)
        col = pl.ds(pl.multiple_of(m * b, b), b)
        home = m // md
        kk = lax.rem(m, md)

        @pl.when(s > 0)
        def _():
            _remote(gbuf.at[m], gbuf.at[m], gsend, grecv.at[m], {'stage': lax.rem(s + ns - 1, ns)}).start()

        @pl.when((s == 0) & (home != 0))
        def _():
            _remote(gbuf.at[m], dx_ref.at[kk], gsend, dxrecv.at[kk], {'stage': home}).start()

        @pl.when((s == 0) & (home == 0))
        def _():
            pltpu.make_async_copy(gbuf.at[m], dx_ref.at[kk], gsend).start()

        pltpu.make_async_copy(dubuf.at[slot], du_ref.at[:, m], dusem.at[slot]).start()
        pltpu.make_async_copy(gtb.at[slot], hg_ref.at[1, :, col], gtsem.at[slot]).start()

    def run(*maths):
        maths = list(maths)
        while maths:
            for g in list(maths):
                if next(g, maths) is maths:
                    maths.remove(g)

    warm = jnp.minimum(1 + 5 * (ns - 1 - s), n)

    def step(t, c):
        mb = t - warm

        @pl.when((t < n) & (t < warm))
        def _():
            fwd_in(t)
            run(fwd_math(t))
            fwd_out(t)

        @pl.when((t < n) & (t >= warm))
        def _():
            fwd_in(t)
            bwd_in(mb)
            run(fwd_math(t), bwd_math(mb))
            fwd_out(t)
            bwd_out(mb)

        @pl.when((t == warm) & (s < 2))
        def _():
            turn(opp)

        @pl.when((t >= n) & (t < warm + n))
        def _():
            bwd_in(mb)
            run(bwd_math(mb))
            bwd_out(mb)

        return c

    lax.fori_loop(0, 2 * n, step, 0)

    @pl.when(s == ns - 1)
    def _():
        pl.semaphore_wait(ygo, 1)
        for home in range(ns - 3, 1, -1):
            for k in range(md):
                _remote(hbuf.at[home * md + k], y_ref.at[k], hsend, yrecv.at[k], {'stage': home}).start()

    for k in range(2):
        pltpu.make_async_copy(abuf.at[k], a_ref.at[:, n - 2 + k], asem.at[k]).wait()
        pltpu.make_async_copy(dubuf.at[k], du_ref.at[:, n - 2 + k], dusem.at[k]).wait()
        pltpu.make_async_copy(htb.at[k], htb.at[k], htsem.at[k]).wait()
        pltpu.make_async_copy(gtb.at[k], gtb.at[k], gtsem.at[k]).wait()
    pltpu.make_async_copy(hbuf, hbuf, hsend).wait()
    pltpu.make_async_copy(gbuf, gbuf, gsend).wait()
    for r in rs + ls + [fr, fl]:
        r.wait_send()
    for k in range(md):
        @pl.when(s != 0)
        def _():
            pltpu.make_async_copy(x_ref.at[k], x_ref.at[k], xsend.at[k]).wait()
            pltpu.make_async_copy(dx_ref.at[k], dx_ref.at[k], dxrecv.at[k]).wait()

        @pl.when(s != ns - 1)
        def _():
            pltpu.make_async_copy(g_ref.at[k], g_ref.at[k], xsend.at[md + k]).wait()
            pltpu.make_async_copy(y_ref.at[k], y_ref.at[k], yrecv.at[k]).wait()


def _wgrad_kernel(ni, nr, hg_ref, a_ref, du_ref, o1_ref, o2_ref,
                  hv, gv, dv, av, s1, s2, r1, r2,
                  lsem, dsem, snd1, snd2, rcv1, rcv2):
    i = lax.axis_index('inner')
    right = lax.rem(i + 1, ni)
    left = lax.rem(i + ni - 1, ni)
    barrier = pltpu.get_barrier_semaphore()
    for nb in (left, right):
        pl.semaphore_signal(barrier, inc=1, device_id={'inner': nb}, device_id_type=MESH)
    def loads(t):
        c1 = lax.rem(i + 2 * ni - 1 - t, ni)
        c2 = lax.rem(i + 1 + t, ni)
        return (pltpu.make_async_copy(du_ref.at[c1], dv.at[t % 2], dsem.at[0, t % 2]),
                pltpu.make_async_copy(a_ref.at[c2], av.at[t % 2], dsem.at[1, t % 2]))

    rows = s1.shape[1]
    k = dv.shape[1] * dv.shape[2]

    def row_loads(r):
        row = pl.ds(pl.multiple_of(r * rows, rows), rows)
        return (pltpu.make_async_copy(hg_ref.at[0, row], hv.at[row], lsem.at[0, r]),
                pltpu.make_async_copy(hg_ref.at[1, row], gv.at[row], lsem.at[1, r]))

    cps = loads(0)
    first = row_loads(0)
    first[0].start()
    cps[0].start()
    first[1].start()
    cps[1].start()
    pl.semaphore_wait(barrier, 2)
    for t in range(ni):
        nxt = loads(t + 1) if t + 1 < ni else None
        slot = t % 2

        def block(r, c):
            row = pl.ds(pl.multiple_of(r * rows, rows), rows)
            if nxt is not None:
                @pl.when(r == 1)
                def _():
                    nxt[0].start()
                    nxt[1].start()
            if t == 0:
                @pl.when(r < nr - 1)
                def _():
                    for cp in row_loads(r + 1):
                        cp.start()
                row_loads(r)[0].wait()

            @pl.when(r == 0)
            def _():
                cps[0].wait()
            p1 = _dot(hv[row, :], dv[slot].reshape(k, dv.shape[3]))
            if t == 0:
                src1 = s1.at[r]
                s1[r] = p1
            else:
                src1 = r1.at[t - 1, r]
                pltpu.make_async_copy(src1, src1, rcv1.at[t - 1, r]).wait()
                if t < ni - 1:
                    r1[t - 1, r] = r1[t - 1, r] + p1
                else:
                    o1_ref[row, :] = r1[t - 1, r] + p1
            if t < ni - 1:
                _remote(src1, r1.at[t, r], snd1, rcv1.at[t, r], {'inner': right}).start()
            if t == 0:
                row_loads(r)[1].wait()

            @pl.when(r == 0)
            def _():
                cps[1].wait()
            p2 = _dot(gv[row, :], av[slot].reshape(k, av.shape[3]))
            if t == 0:
                src2 = s2.at[r]
                s2[r] = p2
            else:
                src2 = r2.at[t - 1, r]
                pltpu.make_async_copy(src2, src2, rcv2.at[t - 1, r]).wait()
                if t < ni - 1:
                    r2[t - 1, r] = r2[t - 1, r] + p2
                else:
                    o2_ref[:, row] = (r2[t - 1, r] + p2).T
            if t < ni - 1:
                _remote(src2, r2.at[t, r], snd2, rcv2.at[t, r], {'inner': left}).start()
            return c

        lax.fori_loop(0, nr, block, 0)
        cps = nxt
    for sem in (snd1, snd2):
        pltpu.make_async_copy(r1, r1, sem).wait()


def _out_kernel(y_ref, dx_ref, w1_ref, w2_ref, yo_ref, dxo_ref, o1_ref, o2_ref, sem):
    cps = [pltpu.make_async_copy(a, o, sem.at[k]) for k, (a, o) in
           enumerate(((w1_ref, o1_ref), (w2_ref, o2_ref), (y_ref, yo_ref), (dx_ref, dxo_ref)))]
    for cp in cps:
        cp.start()
    for cp in cps:
        cp.wait()


def solution(mesh):
    ns = mesh.shape['stage']
    ni = mesh.shape['inner']
    act = P(('data', 'stage', 'inner'), None, None)
    s1 = P(None, 'stage', None, None, 'inner')
    s2 = P(None, 'stage', None, 'inner', None)
    o1 = P('data', 'stage', None, None, 'inner')
    o2 = P('data', 'stage', None, 'inner', None)
    any_ = pl.BlockSpec(memory_space=pl.ANY)
    vmem = pl.BlockSpec(memory_space=pltpu.VMEM)
    dma = pltpu.SemaphoreType.DMA

    def body(x, g, w1, w2):
        md, b, d = x.shape
        f = w1.shape[-1]
        n = ns * md
        sds = jax.ShapeDtypeStruct
        y, dx, hg, a, du = pl.pallas_call(
            functools.partial(_pipe_kernel, ns, ni, md),
            out_shape=(sds((md, b, d), BF16), sds((md, b, d), BF16), sds((2, d, n * b), BF16),
                       sds((ni, n, b, f), BF16), sds((ni, n, b, f), BF16)),
            in_specs=[any_] * 4,
            out_specs=(any_,) * 5,
            scratch_shapes=[
                pltpu.VMEM((ni, d, f), BF16), pltpu.VMEM((ni, f, d), BF16),
                pltpu.VMEM((ni, f, d), BF16), pltpu.VMEM((ni, d, f), BF16),
                pltpu.VMEM((n, b, d), BF16), pltpu.VMEM((n, b, d), BF16),
                pltpu.VMEM((n, ni, b, f), F32),
                pltpu.VMEM((2, d, b), BF16), pltpu.VMEM((2, d, b), BF16),
                pltpu.VMEM((2, ni, b, f), BF16), pltpu.VMEM((2, ni, b, f), BF16),
                dma((6,)), dma((6,)), dma((2,)), dma((2 * md,)), dma((n,)), dma((n,)),
                dma(()), dma(()), dma((md,)), dma((md,)),
                dma((2,)), dma((2,)), dma((2,)), dma((2,)), pltpu.SemaphoreType.REGULAR,
            ],
            compiler_params=pltpu.CompilerParams(collective_id=0, has_side_effects=True, vmem_limit_bytes=63 * 2**20),
            name='pipe',
        )(x, g, w1[0, 0, 0], w2[0, 0, 0])
        nr = d // b
        dw1, dw2 = pl.pallas_call(
            functools.partial(_wgrad_kernel, ni, nr),
            out_shape=(sds((d, f), F32), sds((f, d), F32)),
            in_specs=[any_] * 3,
            out_specs=(vmem, vmem),
            scratch_shapes=[
                pltpu.VMEM((d, n * b), BF16), pltpu.VMEM((d, n * b), BF16),
                pltpu.VMEM((2, n, b, f), BF16), pltpu.VMEM((2, n, b, f), BF16),
                pltpu.VMEM((nr, b, f), F32), pltpu.VMEM((nr, b, f), F32),
                pltpu.VMEM((ni - 1, nr, b, f), F32), pltpu.VMEM((ni - 1, nr, b, f), F32),
                dma((2, nr)), dma((2, 2)), dma(()), dma(()),
                dma((ni - 1, nr)), dma((ni - 1, nr)),
            ],
            compiler_params=pltpu.CompilerParams(collective_id=1, has_side_effects=True, vmem_limit_bytes=48 * 2**20),
            name='wgrad',
        )(hg, a, du)
        y, dx, dw1, dw2 = pl.pallas_call(
            _out_kernel,
            out_shape=(sds(y.shape, BF16), sds(dx.shape, BF16), sds(dw1.shape, F32), sds(dw2.shape, F32)),
            in_specs=[vmem] * 4,
            out_specs=(any_,) * 4,
            scratch_shapes=[dma((4,))],
            compiler_params=pltpu.CompilerParams(vmem_limit_bytes=2**20),
            name='out',
        )(y, dx, dw1, dw2)
        return y, dx, dw1[None, None, None], dw2[None, None, None]

    return jax.shard_map(body, mesh=mesh, in_specs=(act, act, s1, s2), out_specs=(act, act, o1, o2), check_vma=False)
```

```python
import functools

import jax
import jax.numpy as jnp
from jax import lax
from jax.experimental import pallas as pl
from jax.experimental.pallas import tpu as pltpu
from jax.sharding import PartitionSpec as P

MESH = pl.DeviceIdType.MESH
F32 = jnp.float32
BF16 = jnp.bfloat16
C0 = 0.7978845608
C1 = 0.044715


def _dot(a, b):
    return jnp.dot(a, b, preferred_element_type=F32)


def _dot_t(a, b):
    return lax.dot_general(a, b, (((1,), (1,)), ((), ())), preferred_element_type=F32)


def _gate(u):
    return 0.5 + 0.5 * jnp.tanh(u * (C0 + (C0 * C1) * (u * u)))


def _slope(u, p):
    return p * (1.0 + ((1.0 - p) * u) * (2.0 * C0 + (6.0 * C0 * C1) * (u * u)))


def _remote(src, dst, ssem, rsem, dev):
    return pltpu.make_async_remote_copy(src_ref=src, dst_ref=dst, send_sem=ssem, recv_sem=rsem, device_id=dev, device_id_type=MESH)


def _pipe_kernel(ns, ni, md, x_ref, g_ref, w1_ref, w2_ref,
                 y_ref, dx_ref, hg_ref, a_ref, du_ref,
                 w1f, w2f, w1t, w2t, hbuf, gbuf, gp, htb, gtb, abuf, dubuf,
                 wsend, wrecv, wloc, xsend, hrecv, grecv, hsend, gsend, yrecv, dxrecv,
                 htsem, gtsem, asem, dusem, ygo, wgo):
    s = lax.axis_index('stage')
    i = lax.axis_index('inner')
    n = ns * md
    b, d = x_ref.shape[1:]
    f = w1_ref.shape[1]
    right = lax.rem(i + 1, ni)
    left = lax.rem(i + ni - 1, ni)
    opp = lax.rem(i + 2, ni)

    barrier = pltpu.get_barrier_semaphore()
    for k in range(1, ns):
        pl.semaphore_signal(barrier, inc=1, device_id={'stage': lax.rem(s + k, ns)}, device_id_type=MESH)
    for nb in (left, right):
        pl.semaphore_signal(barrier, inc=1, device_id={'inner': nb}, device_id_type=MESH)

    own1 = pltpu.make_async_copy(w1_ref, w1f.at[i], wloc.at[0])
    own2 = pltpu.make_async_copy(w2_ref, w2f.at[i], wloc.at[1])
    own1.start()
    own2.start()
    pl.semaphore_wait(barrier, ns + 1)

    e = d // 4
    lead = [_remote(w1_ref.at[:e], w1f.at[i, :e], wsend.at[6], wrecv.at[0], {'inner': right}),
            _remote(w2_ref.at[:e], w2f.at[i, :e], wsend.at[7], wrecv.at[3], {'inner': left})]
    rs = [_remote(w1_ref.at[e:], w1f.at[i, e:], wsend.at[0], wrecv.at[0], {'inner': right}),
          _remote(w2_ref, w2f.at[i], wsend.at[1], wrecv.at[1], {'inner': right})]
    ls = [_remote(w2_ref.at[e:], w2f.at[i, e:], wsend.at[3], wrecv.at[3], {'inner': left}),
          _remote(w1_ref, w1f.at[i], wsend.at[4], wrecv.at[4], {'inner': left})]

    @pl.when(lax.rem(s, 2) == 1)
    def _():
        pl.semaphore_wait(wgo, 1)

    for r in (lead[0], lead[1], rs[0], ls[0], rs[1], ls[1]):
        r.start()
    for r in lead:
        r.wait_send()

    @pl.when(lax.rem(s, 2) == 0)
    def _():
        pl.semaphore_signal(wgo, inc=1, device_id={'stage': s + 1}, device_id_type=MESH)

    for k in range(md):
        m = lax.rem(s + ns - 1, ns) * md + k

        @pl.when(s == 0)
        def _():
            pltpu.make_async_copy(x_ref.at[k], hbuf.at[m], hrecv.at[m]).start()

        @pl.when(s != 0)
        def _():
            _remote(x_ref.at[k], hbuf.at[m], xsend.at[k], hrecv.at[m], {'stage': 0}).start()

    for k in range(md):
        m = lax.rem(s + ns - 1, ns) * md + k

        @pl.when(s == ns - 1)
        def _():
            pltpu.make_async_copy(g_ref.at[k], gbuf.at[m], grecv.at[m]).start()

        @pl.when(s != ns - 1)
        def _():
            _remote(g_ref.at[k], gbuf.at[m], xsend.at[md + k], grecv.at[m], {'stage': ns - 1}).start()

    def turn(k):
        w1t[k] = w1f[k].T
        w2t[k] = w2f[k].T

    own1.wait()
    own2.wait()
    turn(i)
    pltpu.make_async_copy(w1f.at[left], w1f.at[left], wrecv.at[0]).wait()
    fr = _remote(w1f.at[left], w1f.at[left], wsend.at[2], wrecv.at[2], {'inner': right})
    fr.start()
    pltpu.make_async_copy(w2f.at[right], w2f.at[right], wrecv.at[3]).wait()
    fl = _remote(w2f.at[right], w2f.at[right], wsend.at[5], wrecv.at[5], {'inner': left})
    fl.start()
    pltpu.make_async_copy(w2f.at[left], w2f.at[left], wrecv.at[1]).wait()
    turn(left)
    pltpu.make_async_copy(w1f.at[right], w1f.at[right], wrecv.at[4]).wait()
    turn(right)
    pltpu.make_async_copy(w1f.at[opp], w1f.at[opp], wrecv.at[2]).wait()
    pltpu.make_async_copy(w2f.at[opp], w2f.at[opp], wrecv.at[5]).wait()

    @pl.when(s >= 2)
    def _():
        turn(opp)

    nc = 256

    def fwd_in(m):
        slot = lax.rem(m, 2)
        pltpu.make_async_copy(hbuf.at[m], hbuf.at[m], hrecv.at[m]).wait()

        @pl.when(m >= 2)
        def _():
            pltpu.make_async_copy(abuf.at[slot], a_ref.at[:, m - 2], asem.at[slot]).wait()
            pltpu.make_async_copy(htb.at[slot], htb.at[slot], htsem.at[slot]).wait()

    def fwd_math(m):
        slot = lax.rem(m, 2)
        h = hbuf[m]
        htb[slot] = h.T
        accs = [None] * (d // nc)

        def down(q):
            for c in range(d // nc):
                r = _dot(abuf[slot, q], w2f[q, :, c * nc:(c + 1) * nc])
                accs[c] = r if q == 0 else accs[c] + r

        for q in range(ni):
            for c in range(f // nc):
                cs = slice(c * nc, (c + 1) * nc)
                u = _dot(h, w1f[q, :, cs])
                p = _gate(u)
                abuf[slot, q, :, cs] = (u * p).astype(BF16)
                gp[m, q, :, cs] = _slope(u, p) if q < ni // 2 else u
            if q > 0:
                down(q - 1)
            yield
        down(ni - 1)
        for c in range(d // nc):
            cs = slice(c * nc, (c + 1) * nc)
            hbuf[m, :, cs] = (h[:, cs].astype(F32) + accs[c]).astype(BF16)

    def fwd_out(m):
        slot = lax.rem(m, 2)
        col = pl.ds(pl.multiple_of(m * b, b), b)
        home = lax.rem(m // md + 1, ns)
        kk = lax.rem(m, md)

        @pl.when(s < ns - 1)
        def _():
            _remote(hbuf.at[m], hbuf.at[m], hsend, hrecv.at[m], {'stage': lax.rem(s + 1, ns)}).start()

        @pl.when((s == ns - 1) & ((home == ns - 2) | (home < 2)))
        def _():
            _remote(hbuf.at[m], y_ref.at[kk], hsend, yrecv.at[kk], {'stage': home}).start()

        @pl.when((s == ns - 1) & (home == ns - 1))
        def _():
            pltpu.make_async_copy(hbuf.at[m], y_ref.at[kk], hsend).start()

        pltpu.make_async_copy(abuf.at[slot], a_ref.at[:, m], asem.at[slot]).start()
        pltpu.make_async_copy(htb.at[slot], hg_ref.at[0, :, col], htsem.at[slot]).start()

    def bwd_in(m):
        slot = lax.rem(m, 2)
        pltpu.make_async_copy(gbuf.at[m], gbuf.at[m], grecv.at[m]).wait()

        @pl.when((s == ns - 3) & (m == n - 1))
        def _():
            pl.semaphore_signal(ygo, inc=1, device_id={'stage': ns - 1}, device_id_type=MESH)

        @pl.when(m >= 2)
        def _():
            pltpu.make_async_copy(dubuf.at[slot], du_ref.at[:, m - 2], dusem.at[slot]).wait()
            pltpu.make_async_copy(gtb.at[slot], gtb.at[slot], gtsem.at[slot]).wait()

    def bwd_math(m):
        slot = lax.rem(m, 2)
        g = gbuf[m]
        gtb[slot] = g.T
        accs = [None] * (d // nc)

        def down(q):
            for c in range(d // nc):
                r = _dot(dubuf[slot, q], w1t[q, :, c * nc:(c + 1) * nc])
                accs[c] = r if q == 0 else accs[c] + r

        for q in range(ni):
            for c in range(f // nc):
                cs = slice(c * nc, (c + 1) * nc)
                e = _dot(g, w2t[q, :, cs])
                v = gp[m, q, :, cs]
                if q >= ni // 2:
                    v = _slope(v, _gate(v))
                dubuf[slot, q, :, cs] = (e * v).astype(BF16)
            if q > 0:
                down(q - 1)
            yield
        down(ni - 1)
        for c in range(d // nc):
            cs = slice(c * nc, (c + 1) * nc)
            gbuf[m, :, cs] = (g[:, cs].astype(F32) + accs[c]).astype(BF16)

    def bwd_out(m):
        slot = lax.rem(m, 2)
        col = pl.ds(pl.multiple_of(m * b, b), b)
        home = lax.rem(m // md + 1, ns)
        kk = lax.rem(m, md)

        @pl.when(s > 0)
        def _():
            _remote(gbuf.at[m], gbuf.at[m], gsend, grecv.at[m], {'stage': lax.rem(s + ns - 1, ns)}).start()

        @pl.when((s == 0) & (home != 0))
        def _():
            _remote(gbuf.at[m], dx_ref.at[kk], gsend, dxrecv.at[kk], {'stage': home}).start()

        @pl.when((s == 0) & (home == 0))
        def _():
            pltpu.make_async_copy(gbuf.at[m], dx_ref.at[kk], gsend).start()

        pltpu.make_async_copy(dubuf.at[slot], du_ref.at[:, m], dusem.at[slot]).start()
        pltpu.make_async_copy(gtb.at[slot], hg_ref.at[1, :, col], gtsem.at[slot]).start()

    def run(*maths):
        maths = list(maths)
        while maths:
            for g in list(maths):
                if next(g, maths) is maths:
                    maths.remove(g)

    warm = jnp.minimum(1 + 5 * (ns - 1 - s), n)

    def step(t, c):
        mb = t - warm

        @pl.when((t < n) & (t < warm))
        def _():
            fwd_in(t)
            run(fwd_math(t))
            fwd_out(t)

        @pl.when((t < n) & (t >= warm))
        def _():
            fwd_in(t)
            bwd_in(mb)
            run(fwd_math(t), bwd_math(mb))
            bwd_out(mb)
            fwd_out(t)

        @pl.when((t == warm) & (s < 2))
        def _():
            turn(opp)

        @pl.when((t >= n) & (t < warm + n))
        def _():
            bwd_in(mb)
            run(bwd_math(mb))
            bwd_out(mb)

        return c

    lax.fori_loop(0, 2 * n, step, 0)

    @pl.when(s == ns - 1)
    def _():
        pl.semaphore_wait(ygo, 1)
        for home in range(ns - 3, 1, -1):
            for k in range(md):
                _remote(hbuf.at[(home - 1) * md + k], y_ref.at[k], hsend, yrecv.at[k], {'stage': home}).start()

    for k in range(2):
        pltpu.make_async_copy(abuf.at[k], a_ref.at[:, n - 2 + k], asem.at[k]).wait()
        pltpu.make_async_copy(dubuf.at[k], du_ref.at[:, n - 2 + k], dusem.at[k]).wait()
        pltpu.make_async_copy(htb.at[k], htb.at[k], htsem.at[k]).wait()
        pltpu.make_async_copy(gtb.at[k], gtb.at[k], gtsem.at[k]).wait()
    pltpu.make_async_copy(hbuf, hbuf, hsend).wait()
    pltpu.make_async_copy(gbuf, gbuf, gsend).wait()
    for r in rs + ls + [fr, fl]:
        r.wait_send()
    for k in range(md):
        @pl.when(s != 0)
        def _():
            pltpu.make_async_copy(x_ref.at[k], x_ref.at[k], xsend.at[k]).wait()
            pltpu.make_async_copy(dx_ref.at[k], dx_ref.at[k], dxrecv.at[k]).wait()

        @pl.when(s != ns - 1)
        def _():
            pltpu.make_async_copy(g_ref.at[k], g_ref.at[k], xsend.at[md + k]).wait()
            pltpu.make_async_copy(y_ref.at[k], y_ref.at[k], yrecv.at[k]).wait()


def _wgrad_kernel(ni, nr, hg_ref, a_ref, du_ref, o1_ref, o2_ref,
                  hv, gv, dv, av, s1, s2, r1, r2,
                  lsem, dsem, snd1, snd2, rcv1, rcv2):
    i = lax.axis_index('inner')
    right = lax.rem(i + 1, ni)
    left = lax.rem(i + ni - 1, ni)
    barrier = pltpu.get_barrier_semaphore()
    for nb in (left, right):
        pl.semaphore_signal(barrier, inc=1, device_id={'inner': nb}, device_id_type=MESH)
    def loads(t):
        c1 = lax.rem(i + 2 * ni - 1 - t, ni)
        c2 = lax.rem(i + 1 + t, ni)
        return (pltpu.make_async_copy(du_ref.at[c1], dv.at[t % 2], dsem.at[0, t % 2]),
                pltpu.make_async_copy(a_ref.at[c2], av.at[t % 2], dsem.at[1, t % 2]))

    rows = s1.shape[1]
    k = dv.shape[1] * dv.shape[2]

    def row_loads(r):
        row = pl.ds(pl.multiple_of(r * rows, rows), rows)
        return (pltpu.make_async_copy(hg_ref.at[0, row], hv.at[row], lsem.at[0, r]),
                pltpu.make_async_copy(hg_ref.at[1, row], gv.at[row], lsem.at[1, r]))

    cps = loads(0)
    first = row_loads(0)
    first[0].start()
    cps[0].start()
    first[1].start()
    cps[1].start()
    pl.semaphore_wait(barrier, 2)
    for t in range(ni):
        nxt = loads(t + 1) if t + 1 < ni else None
        slot = t % 2

        def block(r, c):
            row = pl.ds(pl.multiple_of(r * rows, rows), rows)
            if nxt is not None:
                @pl.when(r == 1)
                def _():
                    nxt[0].start()
                    nxt[1].start()
            if t == 0:
                @pl.when(r < nr - 1)
                def _():
                    for cp in row_loads(r + 1):
                        cp.start()
                row_loads(r)[0].wait()

            @pl.when(r == 0)
            def _():
                cps[0].wait()
            p1 = _dot(hv[row, :], dv[slot].reshape(k, dv.shape[3]))
            if t == 0:
                src1 = s1.at[r]
                s1[r] = p1
            else:
                src1 = r1.at[t - 1, r]
                pltpu.make_async_copy(src1, src1, rcv1.at[t - 1, r]).wait()
                if t < ni - 1:
                    r1[t - 1, r] = r1[t - 1, r] + p1
                else:
                    o1_ref[row, :] = r1[t - 1, r] + p1
            if t < ni - 1:
                _remote(src1, r1.at[t, r], snd1, rcv1.at[t, r], {'inner': right}).start()
            if t == 0:
                row_loads(r)[1].wait()

            @pl.when(r == 0)
            def _():
                cps[1].wait()
            p2 = _dot(gv[row, :], av[slot].reshape(k, av.shape[3]))
            if t == 0:
                src2 = s2.at[r]
                s2[r] = p2
            else:
                src2 = r2.at[t - 1, r]
                pltpu.make_async_copy(src2, src2, rcv2.at[t - 1, r]).wait()
                if t < ni - 1:
                    r2[t - 1, r] = r2[t - 1, r] + p2
                else:
                    o2_ref[:, row] = (r2[t - 1, r] + p2).T
            if t < ni - 1:
                _remote(src2, r2.at[t, r], snd2, rcv2.at[t, r], {'inner': left}).start()
            return c

        lax.fori_loop(0, nr, block, 0)
        cps = nxt
    for sem in (snd1, snd2):
        pltpu.make_async_copy(r1, r1, sem).wait()


def _out_kernel(y_ref, dx_ref, w1_ref, w2_ref, yo_ref, dxo_ref, o1_ref, o2_ref, sem):
    cps = [pltpu.make_async_copy(a, o, sem.at[k]) for k, (a, o) in
           enumerate(((w1_ref, o1_ref), (w2_ref, o2_ref), (y_ref, yo_ref), (dx_ref, dxo_ref)))]
    for cp in cps:
        cp.start()
    for cp in cps:
        cp.wait()


def solution(mesh):
    ns = mesh.shape['stage']
    ni = mesh.shape['inner']
    act = P(('data', 'stage', 'inner'), None, None)
    s1 = P(None, 'stage', None, None, 'inner')
    s2 = P(None, 'stage', None, 'inner', None)
    o1 = P('data', 'stage', None, None, 'inner')
    o2 = P('data', 'stage', None, 'inner', None)
    any_ = pl.BlockSpec(memory_space=pl.ANY)
    vmem = pl.BlockSpec(memory_space=pltpu.VMEM)
    dma = pltpu.SemaphoreType.DMA

    def body(x, g, w1, w2):
        md, b, d = x.shape
        f = w1.shape[-1]
        n = ns * md
        sds = jax.ShapeDtypeStruct
        y, dx, hg, a, du = pl.pallas_call(
            functools.partial(_pipe_kernel, ns, ni, md),
            out_shape=(sds((md, b, d), BF16), sds((md, b, d), BF16), sds((2, d, n * b), BF16),
                       sds((ni, n, b, f), BF16), sds((ni, n, b, f), BF16)),
            in_specs=[any_] * 4,
            out_specs=(any_,) * 5,
            scratch_shapes=[
                pltpu.VMEM((ni, d, f), BF16), pltpu.VMEM((ni, f, d), BF16),
                pltpu.VMEM((ni, f, d), BF16), pltpu.VMEM((ni, d, f), BF16),
                pltpu.VMEM((n, b, d), BF16), pltpu.VMEM((n, b, d), BF16),
                pltpu.VMEM((n, ni, b, f), F32),
                pltpu.VMEM((2, d, b), BF16), pltpu.VMEM((2, d, b), BF16),
                pltpu.VMEM((2, ni, b, f), BF16), pltpu.VMEM((2, ni, b, f), BF16),
                dma((8,)), dma((6,)), dma((2,)), dma((2 * md,)), dma((n,)), dma((n,)),
                dma(()), dma(()), dma((md,)), dma((md,)),
                dma((2,)), dma((2,)), dma((2,)), dma((2,)), pltpu.SemaphoreType.REGULAR, pltpu.SemaphoreType.REGULAR,
            ],
            compiler_params=pltpu.CompilerParams(collective_id=0, has_side_effects=True, vmem_limit_bytes=63 * 2**20),
            name='pipe',
        )(x, g, w1[0, 0, 0], w2[0, 0, 0])
        nr = d // b
        dw1, dw2 = pl.pallas_call(
            functools.partial(_wgrad_kernel, ni, nr),
            out_shape=(sds((d, f), F32), sds((f, d), F32)),
            in_specs=[any_] * 3,
            out_specs=(vmem, vmem),
            scratch_shapes=[
                pltpu.VMEM((d, n * b), BF16), pltpu.VMEM((d, n * b), BF16),
                pltpu.VMEM((2, n, b, f), BF16), pltpu.VMEM((2, n, b, f), BF16),
                pltpu.VMEM((nr, b, f), F32), pltpu.VMEM((nr, b, f), F32),
                pltpu.VMEM((ni - 1, nr, b, f), F32), pltpu.VMEM((ni - 1, nr, b, f), F32),
                dma((2, nr)), dma((2, 2)), dma(()), dma(()),
                dma((ni - 1, nr)), dma((ni - 1, nr)),
            ],
            compiler_params=pltpu.CompilerParams(collective_id=1, has_side_effects=True, vmem_limit_bytes=48 * 2**20),
            name='wgrad',
        )(hg, a, du)
        y, dx, dw1, dw2 = pl.pallas_call(
            _out_kernel,
            out_shape=(sds(y.shape, BF16), sds(dx.shape, BF16), sds(dw1.shape, F32), sds(dw2.shape, F32)),
            in_specs=[vmem] * 4,
            out_specs=(any_,) * 4,
            scratch_shapes=[dma((4,))],
            compiler_params=pltpu.CompilerParams(vmem_limit_bytes=2**20),
            name='out',
        )(y, dx, dw1, dw2)
        return y, dx, dw1[None, None, None], dw2[None, None, None]

    return jax.shard_map(body, mesh=mesh, in_specs=(act, act, s1, s2), out_specs=(act, act, o1, o2), check_vma=False)
```

```python
import functools

import jax
import jax.numpy as jnp
from jax import lax
from jax.experimental import pallas as pl
from jax.experimental.pallas import tpu as pltpu
from jax.sharding import PartitionSpec as P

MESH = pl.DeviceIdType.MESH
F32 = jnp.float32
BF16 = jnp.bfloat16
C0 = 0.7978845608
C1 = 0.044715


def _dot(a, b):
    return jnp.dot(a, b, preferred_element_type=F32)


def _dot_t(a, b):
    return lax.dot_general(a, b, (((1,), (1,)), ((), ())), preferred_element_type=F32)


def _gate(u):
    return 0.5 + 0.5 * jnp.tanh(u * (C0 + (C0 * C1) * (u * u)))


def _slope(u, p):
    return p * (1.0 + ((1.0 - p) * u) * (2.0 * C0 + (6.0 * C0 * C1) * (u * u)))


def _remote(src, dst, ssem, rsem, dev):
    return pltpu.make_async_remote_copy(src_ref=src, dst_ref=dst, send_sem=ssem, recv_sem=rsem, device_id=dev, device_id_type=MESH)


def _pipe_kernel(ns, ni, md, x_ref, g_ref, w1_ref, w2_ref,
                 y_ref, dx_ref, hg_ref, a_ref, du_ref,
                 w1f, w2f, w1t, w2t, hbuf, gbuf, gp, htb, gtb, abuf, dubuf,
                 wsend, wrecv, wloc, xsend, hrecv, grecv, hsend, gsend, yrecv, dxrecv,
                 htsem, gtsem, asem, dusem, ygo, wgo):
    s = lax.axis_index('stage')
    i = lax.axis_index('inner')
    n = ns * md
    b, d = x_ref.shape[1:]
    f = w1_ref.shape[1]
    right = lax.rem(i + 1, ni)
    left = lax.rem(i + ni - 1, ni)
    opp = lax.rem(i + 2, ni)

    barrier = pltpu.get_barrier_semaphore()
    for k in range(1, ns):
        pl.semaphore_signal(barrier, inc=1, device_id={'stage': lax.rem(s + k, ns)}, device_id_type=MESH)
    for nb in (left, right):
        pl.semaphore_signal(barrier, inc=1, device_id={'inner': nb}, device_id_type=MESH)

    own1 = pltpu.make_async_copy(w1_ref, w1f.at[i], wloc.at[0])
    own2 = pltpu.make_async_copy(w2_ref, w2f.at[i], wloc.at[1])
    own1.start()
    own2.start()
    pl.semaphore_wait(barrier, ns + 1)

    e = d // 4
    lead = [_remote(w1_ref.at[:e], w1f.at[i, :e], wsend.at[6], wrecv.at[0], {'inner': right}),
            _remote(w2_ref.at[:e], w2f.at[i, :e], wsend.at[7], wrecv.at[3], {'inner': left})]
    rs = [_remote(w1_ref.at[e:], w1f.at[i, e:], wsend.at[0], wrecv.at[0], {'inner': right}),
          _remote(w2_ref, w2f.at[i], wsend.at[1], wrecv.at[1], {'inner': right})]
    ls = [_remote(w2_ref.at[e:], w2f.at[i, e:], wsend.at[3], wrecv.at[3], {'inner': left}),
          _remote(w1_ref, w1f.at[i], wsend.at[4], wrecv.at[4], {'inner': left})]

    @pl.when(lax.rem(s, 2) == 1)
    def _():
        pl.semaphore_wait(wgo, 1)

    for r in (lead[0], lead[1], rs[0], ls[0], rs[1], ls[1]):
        r.start()
    for r in lead:
        r.wait_send()

    @pl.when(lax.rem(s, 2) == 0)
    def _():
        pl.semaphore_signal(wgo, inc=1, device_id={'stage': s + 1}, device_id_type=MESH)

    for k in range(md):
        m = lax.rem(s + ns - 1, ns) * md + k

        @pl.when(s == 0)
        def _():
            pltpu.make_async_copy(x_ref.at[k], hbuf.at[m], hrecv.at[m]).start()

        @pl.when(s != 0)
        def _():
            _remote(x_ref.at[k], hbuf.at[m], xsend.at[k], hrecv.at[m], {'stage': 0}).start()

    for k in range(md):
        m = lax.rem(s + ns - 1, ns) * md + k

        @pl.when(s == ns - 1)
        def _():
            pltpu.make_async_copy(g_ref.at[k], gbuf.at[m], grecv.at[m]).start()

        @pl.when(s != ns - 1)
        def _():
            _remote(g_ref.at[k], gbuf.at[m], xsend.at[md + k], grecv.at[m], {'stage': ns - 1}).start()

    def turn(k):
        w1t[k] = w1f[k].T
        w2t[k] = w2f[k].T

    own1.wait()
    own2.wait()
    turn(i)
    pltpu.make_async_copy(w1f.at[left], w1f.at[left], wrecv.at[0]).wait()
    fr = _remote(w1f.at[left], w1f.at[left], wsend.at[2], wrecv.at[2], {'inner': right})
    fr.start()
    pltpu.make_async_copy(w2f.at[right], w2f.at[right], wrecv.at[3]).wait()
    fl = _remote(w2f.at[right], w2f.at[right], wsend.at[5], wrecv.at[5], {'inner': left})
    fl.start()
    pltpu.make_async_copy(w2f.at[left], w2f.at[left], wrecv.at[1]).wait()
    turn(left)
    pltpu.make_async_copy(w1f.at[right], w1f.at[right], wrecv.at[4]).wait()
    turn(right)
    pltpu.make_async_copy(w1f.at[opp], w1f.at[opp], wrecv.at[2]).wait()
    pltpu.make_async_copy(w2f.at[opp], w2f.at[opp], wrecv.at[5]).wait()

    @pl.when(s >= 2)
    def _():
        turn(opp)

    nc = 256

    def fwd_in(m):
        slot = lax.rem(m, 2)
        pltpu.make_async_copy(hbuf.at[m], hbuf.at[m], hrecv.at[m]).wait()

        @pl.when(m >= 2)
        def _():
            pltpu.make_async_copy(abuf.at[slot], a_ref.at[:, m - 2], asem.at[slot]).wait()
            pltpu.make_async_copy(htb.at[slot], htb.at[slot], htsem.at[slot]).wait()

    def fwd_math(m):
        slot = lax.rem(m, 2)
        h = hbuf[m]
        htb[slot] = h.T
        accs = [None] * (d // nc)

        def down(q):
            for c in range(d // nc):
                r = _dot(abuf[slot, q], w2f[q, :, c * nc:(c + 1) * nc])
                accs[c] = r if q == 0 else accs[c] + r

        for q in range(ni):
            for c in range(f // nc):
                cs = slice(c * nc, (c + 1) * nc)
                u = _dot(h, w1f[q, :, cs])
                p = _gate(u)
                abuf[slot, q, :, cs] = (u * p).astype(BF16)
                gp[m, q, :, cs] = _slope(u, p) if q < ni // 2 else u
            if q > 0:
                down(q - 1)
            yield
        down(ni - 1)
        for c in range(d // nc):
            cs = slice(c * nc, (c + 1) * nc)
            hbuf[m, :, cs] = (h[:, cs].astype(F32) + accs[c]).astype(BF16)

    def fwd_out(m):
        slot = lax.rem(m, 2)
        col = pl.ds(pl.multiple_of(m * b, b), b)
        home = lax.rem(m // md + 1, ns)
        kk = lax.rem(m, md)

        @pl.when(s < ns - 1)
        def _():
            _remote(hbuf.at[m], hbuf.at[m], hsend, hrecv.at[m], {'stage': lax.rem(s + 1, ns)}).start()

        @pl.when((s == ns - 1) & ((home == ns - 2) | (home < 2)))
        def _():
            _remote(hbuf.at[m], y_ref.at[kk], hsend, yrecv.at[kk], {'stage': home}).start()

        @pl.when((s == ns - 1) & (home == ns - 1))
        def _():
            pltpu.make_async_copy(hbuf.at[m], y_ref.at[kk], hsend).start()

        pltpu.make_async_copy(abuf.at[slot], a_ref.at[:, m], asem.at[slot]).start()
        pltpu.make_async_copy(htb.at[slot], hg_ref.at[0, :, col], htsem.at[slot]).start()

    def bwd_in(m):
        slot = lax.rem(m, 2)
        pltpu.make_async_copy(gbuf.at[m], gbuf.at[m], grecv.at[m]).wait()

        @pl.when((s == ns - 3) & (m == n - 1))
        def _():
            pl.semaphore_signal(ygo, inc=1, device_id={'stage': ns - 1}, device_id_type=MESH)

        @pl.when(m >= 2)
        def _():
            pltpu.make_async_copy(dubuf.at[slot], du_ref.at[:, m - 2], dusem.at[slot]).wait()
            pltpu.make_async_copy(gtb.at[slot], gtb.at[slot], gtsem.at[slot]).wait()

    def bwd_math(m):
        slot = lax.rem(m, 2)
        g = gbuf[m]
        gtb[slot] = g.T
        accs = [None] * (d // nc)

        def down(q):
            for c in range(d // nc):
                r = _dot(dubuf[slot, q], w1t[q, :, c * nc:(c + 1) * nc])
                accs[c] = r if q == 0 else accs[c] + r

        for q in range(ni):
            for c in range(f // nc):
                cs = slice(c * nc, (c + 1) * nc)
                e = _dot(g, w2t[q, :, cs])
                v = gp[m, q, :, cs]
                if q >= ni // 2:
                    v = _slope(v, _gate(v))
                dubuf[slot, q, :, cs] = (e * v).astype(BF16)
            if q > 0:
                down(q - 1)
            yield
        down(ni - 1)
        for c in range(d // nc):
            cs = slice(c * nc, (c + 1) * nc)
            gbuf[m, :, cs] = (g[:, cs].astype(F32) + accs[c]).astype(BF16)

    def bwd_out(m):
        slot = lax.rem(m, 2)
        col = pl.ds(pl.multiple_of(m * b, b), b)
        home = lax.rem(m // md + 1, ns)
        kk = lax.rem(m, md)

        @pl.when(s > 0)
        def _():
            _remote(gbuf.at[m], gbuf.at[m], gsend, grecv.at[m], {'stage': lax.rem(s + ns - 1, ns)}).start()

        @pl.when((s == 0) & (home != 0))
        def _():
            _remote(gbuf.at[m], dx_ref.at[kk], gsend, dxrecv.at[kk], {'stage': home}).start()

        @pl.when((s == 0) & (home == 0))
        def _():
            pltpu.make_async_copy(gbuf.at[m], dx_ref.at[kk], gsend).start()

        pltpu.make_async_copy(dubuf.at[slot], du_ref.at[:, m], dusem.at[slot]).start()
        pltpu.make_async_copy(gtb.at[slot], hg_ref.at[1, :, col], gtsem.at[slot]).start()

    def run(*maths):
        maths = list(maths)
        while maths:
            for g in list(maths):
                if next(g, maths) is maths:
                    maths.remove(g)

    warm = jnp.minimum(1 + 5 * (ns - 1 - s), n)

    def step(t, c):
        mb = t - warm

        @pl.when((t < n) & (t < warm))
        def _():
            fwd_in(t)
            run(fwd_math(t))
            fwd_out(t)

        @pl.when((t < n) & (t >= warm))
        def _():
            fwd_in(t)
            bwd_in(mb)
            run(fwd_math(t), bwd_math(mb))
            bwd_out(mb)
            fwd_out(t)

        @pl.when((t == warm) & (s < 2))
        def _():
            turn(opp)

        @pl.when((t >= n) & (t < warm + n))
        def _():
            bwd_in(mb)
            run(bwd_math(mb))
            bwd_out(mb)

        return c

    lax.fori_loop(0, 2 * n, step, 0)

    @pl.when(s == ns - 1)
    def _():
        pl.semaphore_wait(ygo, 1)
        for home in range(ns - 3, 1, -1):
            for k in range(md):
                _remote(hbuf.at[(home - 1) * md + k], y_ref.at[k], hsend, yrecv.at[k], {'stage': home}).start()

    for k in range(2):
        pltpu.make_async_copy(abuf.at[k], a_ref.at[:, n - 2 + k], asem.at[k]).wait()
        pltpu.make_async_copy(dubuf.at[k], du_ref.at[:, n - 2 + k], dusem.at[k]).wait()
        pltpu.make_async_copy(htb.at[k], htb.at[k], htsem.at[k]).wait()
        pltpu.make_async_copy(gtb.at[k], gtb.at[k], gtsem.at[k]).wait()
    pltpu.make_async_copy(hbuf, hbuf, hsend).wait()
    pltpu.make_async_copy(gbuf, gbuf, gsend).wait()
    for r in rs + ls + [fr, fl]:
        r.wait_send()
    for k in range(md):
        @pl.when(s != 0)
        def _():
            pltpu.make_async_copy(x_ref.at[k], x_ref.at[k], xsend.at[k]).wait()
            pltpu.make_async_copy(dx_ref.at[k], dx_ref.at[k], dxrecv.at[k]).wait()

        @pl.when(s != ns - 1)
        def _():
            pltpu.make_async_copy(g_ref.at[k], g_ref.at[k], xsend.at[md + k]).wait()
            pltpu.make_async_copy(y_ref.at[k], y_ref.at[k], yrecv.at[k]).wait()


def _wgrad_kernel(ni, nr, hg_ref, a_ref, du_ref, o1_ref, o2_ref,
                  hv, gv, dv, av, s1, s2, r1, r2,
                  lsem, dsem, snd1, snd2, rcv1, rcv2):
    i = lax.axis_index('inner')
    right = lax.rem(i + 1, ni)
    left = lax.rem(i + ni - 1, ni)
    barrier = pltpu.get_barrier_semaphore()
    for nb in (left, right):
        pl.semaphore_signal(barrier, inc=1, device_id={'inner': nb}, device_id_type=MESH)
    def loads(t):
        c1 = lax.rem(i + 2 * ni - 1 - t, ni)
        c2 = lax.rem(i + 1 + t, ni)
        return (pltpu.make_async_copy(du_ref.at[c1], dv.at[t % 2], dsem.at[0, t % 2]),
                pltpu.make_async_copy(a_ref.at[c2], av.at[t % 2], dsem.at[1, t % 2]))

    rows = s1.shape[1]
    k = dv.shape[1] * dv.shape[2]

    def row_loads(r):
        row = pl.ds(pl.multiple_of(r * rows, rows), rows)
        return (pltpu.make_async_copy(hg_ref.at[0, row], hv.at[row], lsem.at[0, r]),
                pltpu.make_async_copy(hg_ref.at[1, row], gv.at[row], lsem.at[1, r]))

    cps = loads(0)
    first = row_loads(0)
    first[0].start()
    cps[0].start()
    first[1].start()
    cps[1].start()
    pl.semaphore_wait(barrier, 2)
    for t in range(ni):
        nxt = loads(t + 1) if t + 1 < ni else None
        slot = t % 2

        def block(r, c):
            row = pl.ds(pl.multiple_of(r * rows, rows), rows)
            if nxt is not None:
                @pl.when(r == 1)
                def _():
                    nxt[0].start()
                    nxt[1].start()
            if t == 0:
                @pl.when(r < nr - 1)
                def _():
                    for cp in row_loads(r + 1):
                        cp.start()
                row_loads(r)[0].wait()

            @pl.when(r == 0)
            def _():
                cps[0].wait()
                if t > 0:
                    cps[1].wait()
            p1 = _dot(hv[row, :], dv[slot].reshape(k, dv.shape[3]))
            if t > 0:
                p2 = _dot(gv[row, :], av[slot].reshape(k, av.shape[3]))
            if t == 0:
                src1 = s1.at[r]
                s1[r] = p1
            else:
                src1 = r1.at[t - 1, r]
                pltpu.make_async_copy(src1, src1, rcv1.at[t - 1, r]).wait()
                if t < ni - 1:
                    r1[t - 1, r] = r1[t - 1, r] + p1
                else:
                    o1_ref[row, :] = r1[t - 1, r] + p1
            if t < ni - 1:
                _remote(src1, r1.at[t, r], snd1, rcv1.at[t, r], {'inner': right}).start()
            if t == 0:
                row_loads(r)[1].wait()

                @pl.when(r == 0)
                def _():
                    cps[1].wait()
            if t == 0:
                p2 = _dot(gv[row, :], av[slot].reshape(k, av.shape[3]))
                src2 = s2.at[r]
                s2[r] = p2
            else:
                src2 = r2.at[t - 1, r]
                pltpu.make_async_copy(src2, src2, rcv2.at[t - 1, r]).wait()
                if t < ni - 1:
                    r2[t - 1, r] = r2[t - 1, r] + p2
                else:
                    o2_ref[:, row] = (r2[t - 1, r] + p2).T
            if t < ni - 1:
                _remote(src2, r2.at[t, r], snd2, rcv2.at[t, r], {'inner': left}).start()
            return c

        lax.fori_loop(0, nr, block, 0)
        cps = nxt
    for sem in (snd1, snd2):
        pltpu.make_async_copy(r1, r1, sem).wait()


def _out_kernel(y_ref, dx_ref, w1_ref, w2_ref, yo_ref, dxo_ref, o1_ref, o2_ref, sem):
    cps = [pltpu.make_async_copy(a, o, sem.at[k]) for k, (a, o) in
           enumerate(((w1_ref, o1_ref), (w2_ref, o2_ref), (y_ref, yo_ref), (dx_ref, dxo_ref)))]
    for cp in cps:
        cp.start()
    for cp in cps:
        cp.wait()


def solution(mesh):
    ns = mesh.shape['stage']
    ni = mesh.shape['inner']
    act = P(('data', 'stage', 'inner'), None, None)
    s1 = P(None, 'stage', None, None, 'inner')
    s2 = P(None, 'stage', None, 'inner', None)
    o1 = P('data', 'stage', None, None, 'inner')
    o2 = P('data', 'stage', None, 'inner', None)
    any_ = pl.BlockSpec(memory_space=pl.ANY)
    vmem = pl.BlockSpec(memory_space=pltpu.VMEM)
    dma = pltpu.SemaphoreType.DMA

    def body(x, g, w1, w2):
        md, b, d = x.shape
        f = w1.shape[-1]
        n = ns * md
        sds = jax.ShapeDtypeStruct
        y, dx, hg, a, du = pl.pallas_call(
            functools.partial(_pipe_kernel, ns, ni, md),
            out_shape=(sds((md, b, d), BF16), sds((md, b, d), BF16), sds((2, d, n * b), BF16),
                       sds((ni, n, b, f), BF16), sds((ni, n, b, f), BF16)),
            in_specs=[any_] * 4,
            out_specs=(any_,) * 5,
            scratch_shapes=[
                pltpu.VMEM((ni, d, f), BF16), pltpu.VMEM((ni, f, d), BF16),
                pltpu.VMEM((ni, f, d), BF16), pltpu.VMEM((ni, d, f), BF16),
                pltpu.VMEM((n, b, d), BF16), pltpu.VMEM((n, b, d), BF16),
                pltpu.VMEM((n, ni, b, f), F32),
                pltpu.VMEM((2, d, b), BF16), pltpu.VMEM((2, d, b), BF16),
                pltpu.VMEM((2, ni, b, f), BF16), pltpu.VMEM((2, ni, b, f), BF16),
                dma((8,)), dma((6,)), dma((2,)), dma((2 * md,)), dma((n,)), dma((n,)),
                dma(()), dma(()), dma((md,)), dma((md,)),
                dma((2,)), dma((2,)), dma((2,)), dma((2,)), pltpu.SemaphoreType.REGULAR, pltpu.SemaphoreType.REGULAR,
            ],
            compiler_params=pltpu.CompilerParams(collective_id=0, has_side_effects=True, vmem_limit_bytes=63 * 2**20),
            name='pipe',
        )(x, g, w1[0, 0, 0], w2[0, 0, 0])
        nr = d // b
        dw1, dw2 = pl.pallas_call(
            functools.partial(_wgrad_kernel, ni, nr),
            out_shape=(sds((d, f), F32), sds((f, d), F32)),
            in_specs=[any_] * 3,
            out_specs=(vmem, vmem),
            scratch_shapes=[
                pltpu.VMEM((d, n * b), BF16), pltpu.VMEM((d, n * b), BF16),
                pltpu.VMEM((2, n, b, f), BF16), pltpu.VMEM((2, n, b, f), BF16),
                pltpu.VMEM((nr, b, f), F32), pltpu.VMEM((nr, b, f), F32),
                pltpu.VMEM((ni - 1, nr, b, f), F32), pltpu.VMEM((ni - 1, nr, b, f), F32),
                dma((2, nr)), dma((2, 2)), dma(()), dma(()),
                dma((ni - 1, nr)), dma((ni - 1, nr)),
            ],
            compiler_params=pltpu.CompilerParams(collective_id=1, has_side_effects=True, vmem_limit_bytes=48 * 2**20),
            name='wgrad',
        )(hg, a, du)
        y, dx, dw1, dw2 = pl.pallas_call(
            _out_kernel,
            out_shape=(sds(y.shape, BF16), sds(dx.shape, BF16), sds(dw1.shape, F32), sds(dw2.shape, F32)),
            in_specs=[vmem] * 4,
            out_specs=(any_,) * 4,
            scratch_shapes=[dma((4,))],
            compiler_params=pltpu.CompilerParams(vmem_limit_bytes=2**20),
            name='out',
        )(y, dx, dw1, dw2)
        return y, dx, dw1[None, None, None], dw2[None, None, None]

    return jax.shard_map(body, mesh=mesh, in_specs=(act, act, s1, s2), out_specs=(act, act, o1, o2), check_vma=False)
```
